32 devices in a mesh: seq: 8 (over z, y), head: 4 (over x, core).
Axes of the slice: x: 2, y: 2, z: 4, core: 2. Of those that a mesh axis runs over, the one named last changes fastest.
Arguments:
- queries: bfloat16 [1024, 1536], P('seq', 'head'), may hold values from -400 to 400
- latent: bfloat16 [1024, 320], P(('seq', 'head')), may hold values from -6 to 6
- w_kv_up: bfloat16 [256, 2048], P(None, 'head'), may hold values from -0.375 to 0.375
Outputs:
- attended: bfloat16 [1024, 1024], P('seq', 'head')
The draws below stay inside these ranges and needn't reach their ends.
All inputs are finite; a program needn't handle non-finite values.
Results may differ from the reference program's by a relative error of at most 0.004.
Values may be sent and summed in bfloat16 or wider, within the bound.
A program may use at most 64 MiB of HBM per device.

```python
import jax
import jax.numpy as jnp
from jax import lax

D_LATENT = 256
ROPE = 64
NOPE = 128
VDIM = 128
HEADS = 8
TOK_DEV = 128
SEQS = 1
LENGTH = 1024
TOKENS = 1024


def latent_field(key):
    sample = jax.random.normal(jax.random.fold_in(key, 11), (TOKENS, D_LATENT + ROPE), jnp.float32)
    return jnp.clip(sample, -6.0, 6.0)


def draw_latent(key, part):
    return latent_field(key).astype(jnp.bfloat16)


def draw_queries(key, part):
    sample = jax.random.normal(jax.random.fold_in(key, 23), (TOKENS, HEADS, NOPE + ROPE), jnp.float32)
    sample = 2.0 * jnp.clip(sample, -4.0, 4.0)
    return sample.reshape(TOKENS, HEADS * (NOPE + ROPE)).astype(jnp.bfloat16)


def shard_levels(stream_key, extent, cuts, smallest, top_value):
    def one(axis_at, parts):
        heights = jax.random.uniform(jax.random.fold_in(jax.random.fold_in(stream_key, 6), axis_at), (parts,), jnp.float32, smallest / len(cuts), top_value / len(cuts))
        return jnp.repeat(jnp.exp(heights), extent[axis_at] // parts).reshape((-1,) + (1,) * (len(extent) - axis_at - 1))

    loudness = one(*cuts[0])
    for cut in cuts[1:]:
        loudness = loudness * one(*cut)
    return loudness


def scatter_about(own_key, dims, deviation, most, cuts=(), kind=jnp.bfloat16):
    array = jax.random.normal(own_key, dims, jnp.float32) * deviation
    if len(cuts) > 0:
        array = shard_levels(own_key, dims, cuts, -0.22, 0.18) * array
    return jnp.clip(array, min=-most, max=most).astype(kind)


def setup_inputs(seed: int = 0) -> dict:
    keys = jax.random.split(jax.random.key(seed), 4)
    queries = draw_queries(jax.random.fold_in(keys[3], 71), 0)
    latent = draw_latent(jax.random.fold_in(keys[3], 71), 0)
    w_kv_up = scatter_about(keys[2], (D_LATENT, HEADS * (NOPE + VDIM)), D_LATENT ** -0.5, 0.375, ((1, 4),))
    return dict(queries=queries, latent=latent, w_kv_up=w_kv_up)


MASKED = -1e30


def reference(queries, latent, w_kv_up):
    head_width = NOPE + VDIM
    score_scale = (NOPE + ROPE) ** -0.5
    highest = lax.Precision.HIGHEST

    def one_sequence(seq_index):
        first_row = seq_index * LENGTH
        seq_latent = lax.dynamic_slice_in_dim(latent, first_row, LENGTH, 0)
        seq_queries = lax.dynamic_slice_in_dim(queries, first_row, LENGTH, 0)
        key_value = jnp.dot(seq_latent[:, :D_LATENT], w_kv_up, preferred_element_type=jnp.float32)
        key_value = key_value.reshape(LENGTH, HEADS, head_width)
        key_nope = key_value[:, :, :NOPE]
        values = key_value[:, :, NOPE:]
        key_rope = seq_latent[:, D_LATENT:].astype(jnp.float32)
        query_all = seq_queries.reshape(LENGTH, HEADS, NOPE + ROPE).astype(jnp.float32)
        blocks_out = []
        for block_index in range(LENGTH // TOK_DEV):
            low_row = block_index * TOK_DEV
            high_row = low_row + TOK_DEV
            query_block = query_all[low_row:high_row]
            scores = jnp.einsum('qhd,khd->hqk', query_block[:, :, :NOPE], key_nope[:high_row], precision=highest)
            scores = scores + jnp.einsum('qhd,kd->hqk', query_block[:, :, NOPE:], key_rope[:high_row], precision=highest)
            scores = scores * score_scale
            allowed = jnp.arange(high_row)[None, :] <= (low_row + jnp.arange(TOK_DEV))[:, None]
            scores = jnp.where(allowed[None], scores, MASKED)
            row_max = jnp.max(scores, axis=2, keepdims=True)
            weights = jnp.where(allowed[None], jnp.exp(scores - row_max), 0.0)
            totals = jnp.sum(weights, axis=2)
            rounded = lax.optimization_barrier(weights.astype(jnp.bfloat16)).astype(jnp.float32)
            summed = jnp.einsum('hqk,khd->hqd', rounded, values[:high_row], precision=highest)
            result = summed / totals[:, :, None]
            blocks_out.append(jnp.transpose(result, (1, 0, 2)).reshape(TOK_DEV, HEADS * VDIM))
        return jnp.concatenate(blocks_out, axis=0).astype(jnp.bfloat16)

    pieces = lax.map(one_sequence, jnp.arange(SEQS, dtype=jnp.int32))
    return pieces.reshape(TOKENS, HEADS * VDIM)
```

```python
import functools
import math

import jax
import jax.numpy as jnp
from jax import lax
from jax.experimental import pallas as pl
from jax.experimental.pallas import tpu as pltpu
from jax.sharding import PartitionSpec as P

D_LATENT = 256
ROPE = 64
NOPE = 128
VDIM = 128


MASKED = -1e30


def from_behind(shard, axis, by):
    length = lax.axis_size(axis)
    pairs = [(i, i + by) for i in range(length) if 0 <= i + by < length]
    return lax.ppermute(shard, axis, pairs)


def attend(state, key_block, key_start, setup):
    query_side, query_rope, query_pos, w_kv_up, absorb = setup
    numerator, running_max, totals = state
    local_heads = query_rope.shape[1]
    key_count = key_block.shape[0]
    highest = lax.Precision.HIGHEST
    key_latent = key_block[:, :D_LATENT]
    key_rope = key_block[:, D_LATENT:]
    key_value = jnp.dot(key_latent, w_kv_up, preferred_element_type=jnp.float32)
    key_value = key_value.reshape(key_count, local_heads, NOPE + VDIM)
    scores = jnp.einsum("qhd,khd->hqk", query_side, key_value[:, :, :NOPE], precision=highest)
    scores = scores + jnp.einsum(
        "qhd,kd->hqk", query_rope, key_rope, preferred_element_type=jnp.float32
    )
    scores = scores * (NOPE + ROPE) ** (-0.5)
    key_pos = key_start + lax.iota(jnp.int32, key_count)
    allowed = (key_pos[None, :] <= query_pos[:, None]) & (key_pos[None, :] >= 0)
    scores = jnp.where(allowed[None], scores, MASKED)
    new_max = jnp.maximum(running_max, jnp.max(scores, axis=2))
    factor = jnp.exp(running_max - new_max)
    weights = jnp.where(allowed[None], jnp.exp(scores - new_max[:, :, None]), 0.0)
    totals = totals * factor + jnp.sum(weights, axis=2)
    rounded = weights.astype(jnp.bfloat16)
    update = jnp.einsum(
        "hqk,khd->hqd", rounded.astype(jnp.float32), key_value[:, :, NOPE:], precision=highest
    )
    numerator = numerator * factor[:, :, None] + update
    return (numerator, new_max, totals)


def attend_blocks(state, keys, key_start, setup):
    key_total = keys.shape[0]
    block_rows = key_total if key_total <= 1024 else math.gcd(key_total, 1024)
    block_count = key_total // block_rows

    def one_block(block_index, inner):
        offset = block_index * block_rows
        piece = lax.dynamic_slice_in_dim(keys, offset, block_rows, 0)
        return attend(inner, piece, key_start + offset, setup)

    if block_count == 1:
        return one_block(0, state)
    return lax.fori_loop(0, block_count, one_block, state)


def prepare(query_rows, query_pos, w_kv_up):
    row_count = query_rows.shape[0]
    local_heads = w_kv_up.shape[1] // (NOPE + VDIM)
    query_all = query_rows.reshape(row_count, local_heads, NOPE + ROPE)
    query_side = query_all[:, :, :NOPE].astype(jnp.float32)
    width = VDIM
    setup = (query_side, query_all[:, :, NOPE:], query_pos, w_kv_up, False)
    start_state = (
        jnp.zeros((local_heads, row_count, width), jnp.float32),
        jnp.full((local_heads, row_count), MASKED, jnp.float32),
        jnp.zeros((local_heads, row_count), jnp.float32),
    )
    return (setup, start_state)


def finish(state, w_kv_up):
    numerator, running_max, totals = state
    local_heads = w_kv_up.shape[1] // (NOPE + VDIM)
    row_count = totals.shape[1]
    result = numerator / totals[:, :, None]
    return (
        jnp.transpose(result, (1, 0, 2)).reshape(row_count, local_heads * VDIM).astype(jnp.bfloat16)
    )


def body(queries, latent, w_kv_up):
    group_rows = queries.shape[0]
    seq_groups = lax.axis_size("seq")
    group_index = lax.axis_index("seq")
    query_pos = group_index * group_rows + lax.iota(jnp.int32, group_rows)
    setup, state = prepare(queries, query_pos, w_kv_up)
    gathered = lax.all_gather(latent, "head", axis=0, tiled=True)
    state = attend(state, gathered, group_index * group_rows, setup)
    history = gathered
    span_groups = 1
    while span_groups < seq_groups:
        arrived = from_behind(history, "seq", span_groups)
        state = attend_blocks(
            state, arrived, (group_index - 2 * span_groups + 1) * group_rows, setup
        )
        if 2 * span_groups < seq_groups:
            history = jnp.concatenate([arrived, history], axis=0)
        span_groups = span_groups * 2
    return finish(state, w_kv_up)


LOG2E = 1.4426950408889634
MESH = pl.DeviceIdType.MESH
Z_UP, Y_SIDE, X_SIDE, CORE = range(4)


def dot_rows(a, b):
    return lax.dot_general(a, b, (((1,), (1,)), ((), ())), preferred_element_type=jnp.float32)


def halves(x):
    high = x.astype(jnp.bfloat16)
    low = (x - high.astype(jnp.float32)).astype(jnp.bfloat16)
    return high, low


def relay_kernel(
    planes, q_hbm, lat_hbm, w_hbm, out_ref,
    keys, q_ref, w_ref, absorbed, rope, acc, row_max, row_sum,
    load_sem, send_sem, recv_sem,
):
    seq, hd = lax.axis_index("seq"), lax.axis_index("head")
    plane, side = seq // 2, seq % 2
    core = hd % 2
    chunk = lat_hbm.shape[0]
    group = q_ref.shape[0]
    heads = w_ref.shape[1] // (NOPE + VDIM)
    other_side = seq + 1 - 2 * side
    other_pair = (hd + 2) % 4
    other_core = hd + 1 - 2 * core
    targets = {
        Z_UP: (seq + 2, hd),
        Y_SIDE: (other_side, hd),
        X_SIDE: (seq, other_pair),
        CORE: (seq, other_core),
    }

    def copy(s, h, way):
        index = s * 4 + h
        rows = pl.ds(pl.multiple_of(index * chunk, chunk), chunk)
        return pltpu.make_async_remote_copy(
            src_ref=keys.at[rows],
            dst_ref=keys.at[rows],
            send_sem=send_sem.at[index, way],
            recv_sem=recv_sem.at[index],
            device_id=targets[way],
            device_id_type=MESH,
        )

    own_rows = pl.ds(pl.multiple_of((seq * 4 + hd) * chunk, chunk), chunk)
    load_own = pltpu.make_async_copy(lat_hbm, keys.at[own_rows], load_sem.at[0])
    load_q = pltpu.make_async_copy(q_hbm, q_ref, load_sem.at[1])
    load_w = pltpu.make_async_copy(w_hbm, w_ref, load_sem.at[2])
    load_own.start()
    load_q.start()
    load_w.start()

    barrier = pltpu.get_barrier_semaphore()
    for way in (Y_SIDE, X_SIDE, CORE):
        pl.semaphore_signal(barrier, inc=1, device_id=targets[way], device_id_type=MESH)

    @pl.when(plane > 0)
    def _():
        pl.semaphore_signal(barrier, inc=1, device_id=(seq - 2, hd), device_id_type=MESH)

    @pl.when(plane < planes - 1)
    def _():
        pl.semaphore_signal(barrier, inc=1, device_id=(seq + 2, hd), device_id_type=MESH)

    has_below = jnp.where(plane > 0, 1, 0)
    has_above = jnp.where(plane < planes - 1, 1, 0)
    pl.semaphore_wait(barrier, 3 + has_below + has_above)

    def here(k):
        return (plane - k) * 2 + side

    def across(k):
        return (plane - k) * 2 + 1 - side

    def column_sends(k):
        s = here(k)
        return [
            (plane < planes - 1, s, hd, Z_UP),
            (True if k else side == 0, s, hd, Y_SIDE),
            (True, s, hd, X_SIDE),
            (True, s, hd, CORE),
        ]

    def pair_sends(k):
        s = here(k)
        return [
            ((core == 1) if k else (core == 1) & (side == 0), s, other_pair, Y_SIDE),
            (True, s, other_pair, CORE),
        ]

    def side_sends(k):
        s = across(k)
        return [(core == 0, s, hd, X_SIDE), (True, s, hd, CORE)]

    def corner_sends(k):
        return [(True, across(k), other_pair, CORE)]

    def guarded(condition, action):
        if condition is True:
            action()
        else:
            pl.when(condition)(action)

    def start_all(sends):
        for condition, s, h, way in sends:
            guarded(condition, lambda s=s, h=h, way=way: copy(s, h, way).start())

    def drain_all(sends):
        for condition, s, h, way in sends:
            guarded(condition, lambda s=s, h=h, way=way: copy(s, h, way).wait_send())

    def arrived(s, h):
        copy(s, h, CORE).wait_recv()

    def when_plane(k, action):
        guarded(True if k == 0 else plane >= k, action)

    def when_across(k, action):
        guarded(side == 1 if k == 0 else plane >= k, action)

    load_own.wait()
    start_all(column_sends(0))

    load_q.wait()
    load_w.wait()
    for i in range(heads):
        left = i * (NOPE + ROPE)
        key_up = w_ref[:, i * (NOPE + VDIM):i * (NOPE + VDIM) + NOPE]
        mixed = dot_rows(q_ref[:, left:left + NOPE], key_up)
        high, low = halves(mixed)
        absorbed[i * group:(i + 1) * group] = high
        absorbed[(heads + i) * group:(heads + i + 1) * group] = low
        rope[i * group:(i + 1) * group] = q_ref[:, left + NOPE:left + NOPE + ROPE]
    row_max[...] = jnp.full_like(row_max, MASKED)
    row_sum[...] = jnp.zeros_like(row_sum)
    acc[...] = jnp.zeros_like(acc)

    scale = LOG2E * (NOPE + ROPE) ** (-0.5)
    rows = heads * group

    def attend_keys(first_row, count, diagonal):
        block = pl.ds(pl.multiple_of(first_row, count), count)
        lat = keys[block, :D_LATENT]
        both = dot_rows(absorbed[...], lat)
        scores = both[:rows] + both[rows:] + dot_rows(rope[...], keys[block, D_LATENT:])
        scores = scores * scale
        if diagonal:
            q_pos = lax.broadcasted_iota(jnp.int32, (rows, count), 0) % group
            k_pos = lax.broadcasted_iota(jnp.int32, (rows, count), 1)
            allowed = k_pos <= q_pos
            scores = jnp.where(allowed, scores, MASKED)
        old_max = row_max[...]
        new_max = jnp.maximum(old_max, jnp.max(scores, axis=1, keepdims=True))
        factor = jnp.exp2(old_max - new_max)
        weights = jnp.exp2(scores - new_max[:, :1])
        if diagonal:
            weights = jnp.where(allowed, weights, 0.0)
        row_max[...] = new_max
        row_sum[...] = row_sum[...] * factor + jnp.sum(weights, axis=1, keepdims=True)
        update = jnp.dot(weights.astype(jnp.bfloat16), lat, preferred_element_type=jnp.float32)
        acc[...] = acc[...] * factor[:, :1] + update

    def compute(k):
        def own_group():
            for h in (other_core, (other_core + 2) % 4):
                arrived(here(k), h)
            if k == 0:
                attend_keys(seq * group, group, True)

        def other_group():
            for h in (other_core, (other_core + 2) % 4):
                arrived(across(k), h)
            if k == 0:
                attend_keys((seq - 1) * group, group, False)
            else:
                attend_keys((plane - k) * 2 * group, 2 * group, False)

        when_plane(k, own_group)
        when_across(k, other_group)

    for slot in range(1, planes + 3):
        if slot < planes:
            def column(k=slot):
                arrived(here(k), hd)
                start_all(column_sends(k))

            when_plane(slot, column)
        k = slot - 1
        if 0 <= k < planes:
            def pair_part(k=k):
                arrived(here(k), other_pair)
                start_all(pair_sends(k))

            def side_part(k=k):
                arrived(across(k), hd)
                start_all(side_sends(k))

            when_plane(k, pair_part)
            when_across(k, side_part)
        k = slot - 2
        if 0 <= k < planes:
            def corner_part(k=k):
                arrived(across(k), other_pair)
                start_all(corner_sends(k))

            when_across(k, corner_part)
        k = slot - 3
        if 0 <= k < planes:
            compute(k)

    for i in range(heads):
        value_up = w_ref[:, i * (NOPE + VDIM) + NOPE:(i + 1) * (NOPE + VDIM)]
        part = slice(i * group, (i + 1) * group)
        high, low = halves(acc[part])
        result = jnp.dot(high, value_up, preferred_element_type=jnp.float32)
        result = result + jnp.dot(low, value_up, preferred_element_type=jnp.float32)
        out_ref[:, i * VDIM:(i + 1) * VDIM] = (result / row_sum[part, :VDIM]).astype(out_ref.dtype)

    for k in range(planes):
        when_plane(k, lambda k=k: drain_all(column_sends(k) + pair_sends(k)))
        when_across(k, lambda k=k: drain_all(side_sends(k) + corner_sends(k)))


def relay_body(queries, latent, w_kv_up):
    seq_groups = lax.axis_size("seq")
    group = queries.shape[0]
    total = group * seq_groups
    heads = w_kv_up.shape[1] // (NOPE + VDIM)
    rows = heads * group
    chunks = total // latent.shape[0]
    return pl.pallas_call(
        functools.partial(relay_kernel, seq_groups // 2),
        out_shape=jax.ShapeDtypeStruct((group, heads * VDIM), jnp.bfloat16),
        in_specs=[pl.BlockSpec(memory_space=pl.ANY)] * 3,
        out_specs=pl.BlockSpec(memory_space=pltpu.VMEM),
        scratch_shapes=[
            pltpu.VMEM((total, latent.shape[1]), jnp.bfloat16),
            pltpu.VMEM(queries.shape, jnp.bfloat16),
            pltpu.VMEM(w_kv_up.shape, jnp.bfloat16),
            pltpu.VMEM((2 * rows, D_LATENT), jnp.bfloat16),
            pltpu.VMEM((rows, ROPE), jnp.bfloat16),
            pltpu.VMEM((rows, D_LATENT), jnp.float32),
            pltpu.VMEM((rows, 128), jnp.float32),
            pltpu.VMEM((rows, 128), jnp.float32),
            pltpu.SemaphoreType.DMA((3,)),
            pltpu.SemaphoreType.DMA((chunks, 4)),
            pltpu.SemaphoreType.DMA((chunks,)),
        ],
        compiler_params=pltpu.CompilerParams(collective_id=0, has_side_effects=True),
    )(queries, latent, w_kv_up)


def solution(mesh):
    in_specs = (P("seq", "head"), P(("seq", "head"), None), P(None, "head"))
    out_specs = P("seq", "head")
    small = mesh.shape["seq"] <= 16 and mesh.shape["seq"] % 2 == 0 and mesh.shape["head"] == 4
    chosen = relay_body if small else body
    return jax.shard_map(chosen, mesh=mesh, in_specs=in_specs, out_specs=out_specs, check_vma=False)
```

```python
import functools
import math

import jax
import jax.numpy as jnp
from jax import lax
from jax.experimental import pallas as pl
from jax.experimental.pallas import tpu as pltpu
from jax.sharding import PartitionSpec as P

D_LATENT = 256
ROPE = 64
NOPE = 128
VDIM = 128


MASKED = -1e30


def from_behind(shard, axis, by):
    length = lax.axis_size(axis)
    pairs = [(i, i + by) for i in range(length) if 0 <= i + by < length]
    return lax.ppermute(shard, axis, pairs)


def attend(state, key_block, key_start, setup):
    query_side, query_rope, query_pos, w_kv_up, absorb = setup
    numerator, running_max, totals = state
    local_heads = query_rope.shape[1]
    key_count = key_block.shape[0]
    highest = lax.Precision.HIGHEST
    key_latent = key_block[:, :D_LATENT]
    key_rope = key_block[:, D_LATENT:]
    key_value = jnp.dot(key_latent, w_kv_up, preferred_element_type=jnp.float32)
    key_value = key_value.reshape(key_count, local_heads, NOPE + VDIM)
    scores = jnp.einsum("qhd,khd->hqk", query_side, key_value[:, :, :NOPE], precision=highest)
    scores = scores + jnp.einsum(
        "qhd,kd->hqk", query_rope, key_rope, preferred_element_type=jnp.float32
    )
    scores = scores * (NOPE + ROPE) ** (-0.5)
    key_pos = key_start + lax.iota(jnp.int32, key_count)
    allowed = (key_pos[None, :] <= query_pos[:, None]) & (key_pos[None, :] >= 0)
    scores = jnp.where(allowed[None], scores, MASKED)
    new_max = jnp.maximum(running_max, jnp.max(scores, axis=2))
    factor = jnp.exp(running_max - new_max)
    weights = jnp.where(allowed[None], jnp.exp(scores - new_max[:, :, None]), 0.0)
    totals = totals * factor + jnp.sum(weights, axis=2)
    rounded = weights.astype(jnp.bfloat16)
    update = jnp.einsum(
        "hqk,khd->hqd", rounded.astype(jnp.float32), key_value[:, :, NOPE:], precision=highest
    )
    numerator = numerator * factor[:, :, None] + update
    return (numerator, new_max, totals)


def attend_blocks(state, keys, key_start, setup):
    key_total = keys.shape[0]
    block_rows = key_total if key_total <= 1024 else math.gcd(key_total, 1024)
    block_count = key_total // block_rows

    def one_block(block_index, inner):
        offset = block_index * block_rows
        piece = lax.dynamic_slice_in_dim(keys, offset, block_rows, 0)
        return attend(inner, piece, key_start + offset, setup)

    if block_count == 1:
        return one_block(0, state)
    return lax.fori_loop(0, block_count, one_block, state)


def prepare(query_rows, query_pos, w_kv_up):
    row_count = query_rows.shape[0]
    local_heads = w_kv_up.shape[1] // (NOPE + VDIM)
    query_all = query_rows.reshape(row_count, local_heads, NOPE + ROPE)
    query_side = query_all[:, :, :NOPE].astype(jnp.float32)
    width = VDIM
    setup = (query_side, query_all[:, :, NOPE:], query_pos, w_kv_up, False)
    start_state = (
        jnp.zeros((local_heads, row_count, width), jnp.float32),
        jnp.full((local_heads, row_count), MASKED, jnp.float32),
        jnp.zeros((local_heads, row_count), jnp.float32),
    )
    return (setup, start_state)


def finish(state, w_kv_up):
    numerator, running_max, totals = state
    local_heads = w_kv_up.shape[1] // (NOPE + VDIM)
    row_count = totals.shape[1]
    result = numerator / totals[:, :, None]
    return (
        jnp.transpose(result, (1, 0, 2)).reshape(row_count, local_heads * VDIM).astype(jnp.bfloat16)
    )


def body(queries, latent, w_kv_up):
    group_rows = queries.shape[0]
    seq_groups = lax.axis_size("seq")
    group_index = lax.axis_index("seq")
    query_pos = group_index * group_rows + lax.iota(jnp.int32, group_rows)
    setup, state = prepare(queries, query_pos, w_kv_up)
    gathered = lax.all_gather(latent, "head", axis=0, tiled=True)
    state = attend(state, gathered, group_index * group_rows, setup)
    history = gathered
    span_groups = 1
    while span_groups < seq_groups:
        arrived = from_behind(history, "seq", span_groups)
        state = attend_blocks(
            state, arrived, (group_index - 2 * span_groups + 1) * group_rows, setup
        )
        if 2 * span_groups < seq_groups:
            history = jnp.concatenate([arrived, history], axis=0)
        span_groups = span_groups * 2
    return finish(state, w_kv_up)


LOG2E = 1.4426950408889634
MESH = pl.DeviceIdType.MESH
def dot_rows(a, b):
    return lax.dot_general(a, b, (((1,), (1,)), ((), ())), preferred_element_type=jnp.float32)


def halves(x):
    high = x.astype(jnp.bfloat16)
    low = (x - high.astype(jnp.float32)).astype(jnp.bfloat16)
    return high, low


def relay_kernel(
    planes, q_hbm, lat_hbm, w_hbm, out_ref,
    keys, q_ref, w_ref, absorbed, rope, acc, row_max, row_sum,
    load_sem, send_sem, recv_sem,
):
    seq, hd = lax.axis_index("seq"), lax.axis_index("head")
    plane, side = seq // 2, seq % 2
    pair, core = hd // 2, hd % 2
    chunk = lat_hbm.shape[0]
    group = q_ref.shape[0]
    heads = w_ref.shape[1] // (NOPE + VDIM)
    across = seq + 1 - 2 * side
    other_pair = 1 - pair
    other_core = 1 - core

    def slot_of(s, p, c):
        return (c * planes * 2 + s) * 2 + p

    def copy(index, target_seq, target_head, way):
        rows = pl.ds(pl.multiple_of(index * chunk, chunk), chunk)
        return pltpu.make_async_remote_copy(
            src_ref=keys.at[rows],
            dst_ref=keys.at[rows],
            send_sem=send_sem.at[index, way],
            recv_sem=recv_sem.at[index],
            device_id=(target_seq, target_head),
            device_id_type=MESH,
        )

    own = slot_of(seq, pair, core)
    own_rows = pl.ds(pl.multiple_of(own * chunk, chunk), chunk)
    load_own = pltpu.make_async_copy(lat_hbm, keys.at[own_rows], load_sem.at[0])
    load_q = pltpu.make_async_copy(q_hbm, q_ref, load_sem.at[1])
    load_w = pltpu.make_async_copy(w_hbm, w_ref, load_sem.at[2])
    load_own.start()

    in_plane = [
        (across, other_pair * 2 + core),
        (across, hd),
        (seq, other_pair * 2 + core),
        (seq, pair * 2 + other_core),
    ]
    barrier = pltpu.get_barrier_semaphore()
    for gap in range(planes - 1, 0, -1):
        @pl.when(plane >= gap)
        def _(gap=gap):
            pl.semaphore_signal(
                barrier, inc=1, device_id=(seq - 2 * gap, hd), device_id_type=MESH
            )
    for target in in_plane:
        pl.semaphore_signal(barrier, inc=1, device_id=target, device_id_type=MESH)
    load_q.start()
    load_w.start()
    pl.semaphore_wait(barrier, len(in_plane) + planes - 1 - plane)

    def guarded(condition, action):
        if condition is True:
            action()
        else:
            pl.when(condition)(action)

    def climb_sends():
        return [
            (plane + gap < planes, copy(own, seq + 2 * gap, hd, gap + 3))
            for gap in range(planes - 1, 0, -1)
        ]

    def plane_sends(k):
        index = slot_of(seq - 2 * k, pair, core)
        to_across = True if k else side == 0
        flags = (to_across, to_across, True, True)
        return [
            (flag, copy(index, target[0], target[1], way))
            for way, (flag, target) in enumerate(zip(flags, in_plane))
        ]

    def core_send(index):
        return (True, copy(index, in_plane[3][0], in_plane[3][1], 3))

    def own_pair_sends(k):
        return [core_send(slot_of(seq - 2 * k, other_pair, core))]

    def across_sends(k):
        return [core_send(slot_of(across - 2 * k, p, core)) for p in (pair, other_pair)]

    def start_all(sends):
        for condition, item in sends:
            guarded(condition, item.start)

    def drain_all(sends):
        for condition, item in sends:
            guarded(condition, item.wait_send)

    def arrived(index):
        copy(index, in_plane[3][0], in_plane[3][1], 3).wait_recv()

    def when_plane(k, action):
        guarded(True if k == 0 else plane >= k, action)

    def when_across(k, action):
        guarded(side == 1 if k == 0 else plane >= k, action)

    load_own.wait()
    start_all(climb_sends())
    start_all(plane_sends(0))

    load_q.wait()
    load_w.wait()
    for i in range(heads):
        left = i * (NOPE + ROPE)
        key_up = w_ref[:, i * (NOPE + VDIM):i * (NOPE + VDIM) + NOPE]
        mixed = dot_rows(q_ref[:, left:left + NOPE], key_up)
        high, low = halves(mixed)
        absorbed[i * group:(i + 1) * group] = high
        absorbed[(heads + i) * group:(heads + i + 1) * group] = low
        rope[i * group:(i + 1) * group] = q_ref[:, left + NOPE:left + NOPE + ROPE]
    row_max[...] = jnp.full_like(row_max, MASKED)
    row_sum[...] = jnp.zeros_like(row_sum)
    acc[...] = jnp.zeros_like(acc)

    scale = LOG2E * (NOPE + ROPE) ** (-0.5)
    rows = heads * group

    def attend_keys(first_slot, slots, key_core, diagonal):
        count = slots * chunk
        block = pl.ds(pl.multiple_of(first_slot * chunk, chunk), count)
        lat = keys[block, :D_LATENT]
        both = dot_rows(absorbed[...], lat)
        scores = both[:rows] + both[rows:] + dot_rows(rope[...], keys[block, D_LATENT:])
        scores = scores * scale
        if diagonal:
            q_pos = lax.broadcasted_iota(jnp.int32, (rows, count), 0) % group
            q_pos = q_pos + (slots // 2 - 1) * group
            k_row = lax.broadcasted_iota(jnp.int32, (rows, count), 1)
            k_pos = (k_row // chunk * 2 + key_core) * chunk + k_row % chunk
            allowed = k_pos <= q_pos
            scores = jnp.where(allowed, scores, MASKED)
        old_max = row_max[...]
        new_max = jnp.maximum(old_max, jnp.max(scores, axis=1, keepdims=True))
        factor = jnp.exp2(old_max - new_max)
        weights = jnp.exp2(scores - new_max[:, :1])
        if diagonal:
            weights = jnp.where(allowed, weights, 0.0)
        row_max[...] = new_max
        row_sum[...] = row_sum[...] * factor + jnp.sum(weights, axis=1, keepdims=True)
        update = jnp.dot(weights.astype(jnp.bfloat16), lat, preferred_element_type=jnp.float32)
        acc[...] = acc[...] * factor[:, :1] + update

    def compute(k, key_core):
        first = slot_of((plane - k) * 2, 0, key_core)
        if k == 0:
            pl.when(side == 0)(lambda: attend_keys(first, 2, key_core, True))
            pl.when(side == 1)(lambda: attend_keys(first, 4, key_core, True))
        else:
            pl.when(plane >= k)(lambda: attend_keys(first, 4, key_core, False))

    def from_below(k):
        def action():
            arrived(slot_of(seq - 2 * k, pair, core))
            start_all(plane_sends(k))

        when_plane(k, action)

    def from_plane(k):
        def own_side():
            arrived(slot_of(seq - 2 * k, other_pair, core))
            start_all(own_pair_sends(k))

        def other_side():
            for p in (pair, other_pair):
                arrived(slot_of(across - 2 * k, p, core))
            start_all(across_sends(k))

        when_plane(k, own_side)
        when_across(k, other_side)

    def from_core(k):
        def own_side():
            for p in (pair, other_pair):
                arrived(slot_of(seq - 2 * k, p, other_core))

        def other_side():
            for p in (pair, other_pair):
                arrived(slot_of(across - 2 * k, p, other_core))

        when_plane(k, own_side)
        when_across(k, other_side)

    for k in range(1, planes):
        if k == 2:
            from_plane(0)
        from_below(k)
    if planes < 3:
        from_plane(0)
    compute(0, core)
    for k in range(1, planes):
        from_plane(k)
        from_core(k - 1)
        compute(k - 1, other_core)
        compute(k, core)
    from_core(planes - 1)
    compute(planes - 1, other_core)

    for i in range(heads):
        value_up = w_ref[:, i * (NOPE + VDIM) + NOPE:(i + 1) * (NOPE + VDIM)]
        part = slice(i * group, (i + 1) * group)
        high, low = halves(acc[part])
        result = jnp.dot(high, value_up, preferred_element_type=jnp.float32)
        result = result + jnp.dot(low, value_up, preferred_element_type=jnp.float32)
        out_ref[:, i * VDIM:(i + 1) * VDIM] = (result / row_sum[part, :VDIM]).astype(out_ref.dtype)

    drain_all(climb_sends())
    for k in range(planes):
        when_plane(k, lambda k=k: drain_all(plane_sends(k) + own_pair_sends(k)))
        when_across(k, lambda k=k: drain_all(across_sends(k)))


def relay_body(queries, latent, w_kv_up):
    seq_groups = lax.axis_size("seq")
    group = queries.shape[0]
    total = group * seq_groups
    heads = w_kv_up.shape[1] // (NOPE + VDIM)
    rows = heads * group
    chunks = total // latent.shape[0]
    return pl.pallas_call(
        functools.partial(relay_kernel, seq_groups // 2),
        out_shape=pltpu.VMEM((group, heads * VDIM), jnp.bfloat16),
        in_specs=[pl.BlockSpec(memory_space=pltpu.HBM)] * 3,
        out_specs=pl.BlockSpec(memory_space=pltpu.VMEM),
        scratch_shapes=[
            pltpu.VMEM((total, latent.shape[1]), jnp.bfloat16),
            pltpu.VMEM(queries.shape, jnp.bfloat16),
            pltpu.VMEM(w_kv_up.shape, jnp.bfloat16),
            pltpu.VMEM((2 * rows, D_LATENT), jnp.bfloat16),
            pltpu.VMEM((rows, ROPE), jnp.bfloat16),
            pltpu.VMEM((rows, D_LATENT), jnp.float32),
            pltpu.VMEM((rows, 128), jnp.float32),
            pltpu.VMEM((rows, 128), jnp.float32),
            pltpu.SemaphoreType.DMA((3,)),
            pltpu.SemaphoreType.DMA((chunks, seq_groups // 2 + 3)),
            pltpu.SemaphoreType.DMA((chunks,)),
        ],
        compiler_params=pltpu.CompilerParams(collective_id=0, has_side_effects=True),
    )(queries, latent, w_kv_up)


def solution(mesh):
    in_specs = (P("seq", "head"), P(("seq", "head"), None), P(None, "head"))
    out_specs = P("seq", "head")
    small = mesh.shape["seq"] <= 16 and mesh.shape["seq"] % 2 == 0 and mesh.shape["head"] == 4
    chosen = relay_body if small else body
    return jax.shard_map(chosen, mesh=mesh, in_specs=in_specs, out_specs=out_specs, check_vma=False)
```

```python
import functools
import math

import jax
import jax.numpy as jnp
from jax import lax
from jax.experimental import pallas as pl
from jax.experimental.pallas import tpu as pltpu
from jax.sharding import PartitionSpec as P

D_LATENT = 256
ROPE = 64
NOPE = 128
VDIM = 128


MASKED = -1e30


def from_behind(shard, axis, by):
    length = lax.axis_size(axis)
    pairs = [(i, i + by) for i in range(length) if 0 <= i + by < length]
    return lax.ppermute(shard, axis, pairs)


def attend(state, key_block, key_start, setup):
    query_side, query_rope, query_pos, w_kv_up, absorb = setup
    numerator, running_max, totals = state
    local_heads = query_rope.shape[1]
    key_count = key_block.shape[0]
    highest = lax.Precision.HIGHEST
    key_latent = key_block[:, :D_LATENT]
    key_rope = key_block[:, D_LATENT:]
    key_value = jnp.dot(key_latent, w_kv_up, preferred_element_type=jnp.float32)
    key_value = key_value.reshape(key_count, local_heads, NOPE + VDIM)
    scores = jnp.einsum("qhd,khd->hqk", query_side, key_value[:, :, :NOPE], precision=highest)
    scores = scores + jnp.einsum(
        "qhd,kd->hqk", query_rope, key_rope, preferred_element_type=jnp.float32
    )
    scores = scores * (NOPE + ROPE) ** (-0.5)
    key_pos = key_start + lax.iota(jnp.int32, key_count)
    allowed = (key_pos[None, :] <= query_pos[:, None]) & (key_pos[None, :] >= 0)
    scores = jnp.where(allowed[None], scores, MASKED)
    new_max = jnp.maximum(running_max, jnp.max(scores, axis=2))
    factor = jnp.exp(running_max - new_max)
    weights = jnp.where(allowed[None], jnp.exp(scores - new_max[:, :, None]), 0.0)
    totals = totals * factor + jnp.sum(weights, axis=2)
    rounded = weights.astype(jnp.bfloat16)
    update = jnp.einsum(
        "hqk,khd->hqd", rounded.astype(jnp.float32), key_value[:, :, NOPE:], precision=highest
    )
    numerator = numerator * factor[:, :, None] + update
    return (numerator, new_max, totals)


def attend_blocks(state, keys, key_start, setup):
    key_total = keys.shape[0]
    block_rows = key_total if key_total <= 1024 else math.gcd(key_total, 1024)
    block_count = key_total // block_rows

    def one_block(block_index, inner):
        offset = block_index * block_rows
        piece = lax.dynamic_slice_in_dim(keys, offset, block_rows, 0)
        return attend(inner, piece, key_start + offset, setup)

    if block_count == 1:
        return one_block(0, state)
    return lax.fori_loop(0, block_count, one_block, state)


def prepare(query_rows, query_pos, w_kv_up):
    row_count = query_rows.shape[0]
    local_heads = w_kv_up.shape[1] // (NOPE + VDIM)
    query_all = query_rows.reshape(row_count, local_heads, NOPE + ROPE)
    query_side = query_all[:, :, :NOPE].astype(jnp.float32)
    width = VDIM
    setup = (query_side, query_all[:, :, NOPE:], query_pos, w_kv_up, False)
    start_state = (
        jnp.zeros((local_heads, row_count, width), jnp.float32),
        jnp.full((local_heads, row_count), MASKED, jnp.float32),
        jnp.zeros((local_heads, row_count), jnp.float32),
    )
    return (setup, start_state)


def finish(state, w_kv_up):
    numerator, running_max, totals = state
    local_heads = w_kv_up.shape[1] // (NOPE + VDIM)
    row_count = totals.shape[1]
    result = numerator / totals[:, :, None]
    return (
        jnp.transpose(result, (1, 0, 2)).reshape(row_count, local_heads * VDIM).astype(jnp.bfloat16)
    )


def body(queries, latent, w_kv_up):
    group_rows = queries.shape[0]
    seq_groups = lax.axis_size("seq")
    group_index = lax.axis_index("seq")
    query_pos = group_index * group_rows + lax.iota(jnp.int32, group_rows)
    setup, state = prepare(queries, query_pos, w_kv_up)
    gathered = lax.all_gather(latent, "head", axis=0, tiled=True)
    state = attend(state, gathered, group_index * group_rows, setup)
    history = gathered
    span_groups = 1
    while span_groups < seq_groups:
        arrived = from_behind(history, "seq", span_groups)
        state = attend_blocks(
            state, arrived, (group_index - 2 * span_groups + 1) * group_rows, setup
        )
        if 2 * span_groups < seq_groups:
            history = jnp.concatenate([arrived, history], axis=0)
        span_groups = span_groups * 2
    return finish(state, w_kv_up)


LOG2E = 1.4426950408889634
MESH = pl.DeviceIdType.MESH
def dot_rows(a, b):
    return lax.dot_general(a, b, (((1,), (1,)), ((), ())), preferred_element_type=jnp.float32)


def halves(x):
    high = x.astype(jnp.bfloat16)
    low = (x - high.astype(jnp.float32)).astype(jnp.bfloat16)
    return high, low


def relay_kernel(
    planes, q_hbm, lat_hbm, w_hbm, out_ref,
    keys, q_ref, w_ref, absorbed, rope, acc, row_max, row_sum,
    load_sem, climb_sem, send_sem, recv_sem, ready_sem,
):
    seq, hd = lax.axis_index("seq"), lax.axis_index("head")
    plane, side = seq // 2, seq % 2
    pair, core = hd // 2, hd % 2
    chunk = lat_hbm.shape[0]
    group = q_ref.shape[0]
    heads = w_ref.shape[1] // (NOPE + VDIM)
    across = seq + 1 - 2 * side
    other_pair = 1 - pair
    other_core = 1 - core

    def slot_of(s, p, c):
        return (c * planes * 2 + s) * 2 + p

    def region(index, count):
        return keys.at[pl.ds(pl.multiple_of(index * chunk, chunk), count * chunk)]

    def copy(index, target, sent, landed, count=1):
        return pltpu.make_async_remote_copy(
            src_ref=region(index, count),
            dst_ref=region(index, count),
            send_sem=sent,
            recv_sem=landed,
            device_id=target,
            device_id_type=MESH,
        )

    own = slot_of(seq, pair, core)
    own_rows = pl.ds(pl.multiple_of(own * chunk, chunk), chunk)
    load_own = pltpu.make_async_copy(lat_hbm, keys.at[own_rows], load_sem.at[0])
    load_q = pltpu.make_async_copy(q_hbm, q_ref, load_sem.at[1])
    load_w = pltpu.make_async_copy(w_hbm, w_ref, load_sem.at[2])
    load_own.start()

    across_peer = (across, hd)
    pair_peer = (seq, other_pair * 2 + core)
    corner_peer = (across, other_pair * 2 + core)
    core_peer = (seq, pair * 2 + other_core)
    below, above = (seq - 2, hd), (seq + 2, hd)
    has_below, has_above = plane > 0, plane < planes - 1

    barrier = pltpu.get_barrier_semaphore()

    @pl.when(has_below)
    def _():
        pl.semaphore_signal(barrier, inc=1, device_id=below, device_id_type=MESH)

    for target in (pair_peer, across_peer, core_peer):
        pl.semaphore_signal(barrier, inc=1, device_id=target, device_id_type=MESH)

    @pl.when(has_above)
    def _():
        pl.semaphore_signal(barrier, inc=1, device_id=above, device_id_type=MESH)

    load_q.start()
    load_w.start()
    pl.semaphore_wait(barrier, 3 + jnp.where(has_below, 1, 0) + jnp.where(has_above, 1, 0))

    def pass_down(gap):
        pl.semaphore_signal(ready_sem.at[gap], inc=1, device_id=below, device_id_type=MESH)

    if planes > 2:
        pl.when(has_below & has_above)(lambda: pass_down(2))
    pl.semaphore_signal(ready_sem.at[0], inc=1, device_id=pair_peer, device_id_type=MESH)

    def guarded(condition, action):
        if condition is True:
            action()
        else:
            pl.when(condition)(action)

    BELOW, PAIR, ACROSS, CORNER, CORE = range(5)

    def climb(gap):
        return copy(own, (seq + 2 * gap, hd), climb_sem.at[gap], recv_sem.at[gap, BELOW])

    def send(index, k, target, kind):
        copy(index, target, send_sem.at[k], recv_sem.at[k, kind]).start()

    def send_sides(k):
        index = slot_of(seq - 2 * k, pair, core)
        guarded(True if k else side == 0, lambda: send(index, k, across_peer, ACROSS))
        send(index, k, pair_peer, PAIR)
        send(index, k, core_peer, CORE)

    def send_corner(k):
        index = slot_of(seq - 2 * k, pair, core)
        guarded(True if k else side == 0, lambda: send(index, k, corner_peer, CORNER))

    def arrived(index, k, kind, count=1):
        copy(index, core_peer, send_sem.at[k], recv_sem.at[k, kind], count).wait_recv()

    def when_plane(k, action):
        guarded(True if k == 0 else plane >= k, action)

    def when_across(k, action):
        guarded(side == 1 if k == 0 else plane >= k, action)

    load_own.wait()
    if planes > 1:
        pl.when(has_above)(lambda: climb(1).start())
    send_sides(0)
    pl.semaphore_wait(ready_sem.at[0], 1)
    send_corner(0)
    for gap in range(2, planes):
        @pl.when(plane + gap < planes)
        def _(gap=gap):
            pl.semaphore_wait(ready_sem.at[gap], 1)
            if gap + 1 < planes:
                pl.when(has_below)(lambda: pass_down(gap + 1))
            climb(gap).start()

    load_q.wait()
    load_w.wait()
    for i in range(heads):
        left = i * (NOPE + ROPE)
        key_up = w_ref[:, i * (NOPE + VDIM):i * (NOPE + VDIM) + NOPE]
        mixed = dot_rows(q_ref[:, left:left + NOPE], key_up)
        high, low = halves(mixed)
        absorbed[i * group:(i + 1) * group] = high
        absorbed[(heads + i) * group:(heads + i + 1) * group] = low
        rope[i * group:(i + 1) * group] = q_ref[:, left + NOPE:left + NOPE + ROPE]
    row_max[...] = jnp.full_like(row_max, MASKED)
    row_sum[...] = jnp.zeros_like(row_sum)
    acc[...] = jnp.zeros_like(acc)

    scale = LOG2E * (NOPE + ROPE) ** (-0.5)
    rows = heads * group

    def attend_keys(first_slot, slots, key_core, diagonal):
        count = slots * chunk
        block = pl.ds(pl.multiple_of(first_slot * chunk, chunk), count)
        lat = keys[block, :D_LATENT]
        both = dot_rows(absorbed[...], lat)
        scores = both[:rows] + both[rows:] + dot_rows(rope[...], keys[block, D_LATENT:])
        scores = scores * scale
        if diagonal:
            q_pos = lax.broadcasted_iota(jnp.int32, (rows, count), 0) % group
            q_pos = q_pos + (slots // 2 - 1) * group
            k_row = lax.broadcasted_iota(jnp.int32, (rows, count), 1)
            k_pos = (k_row // chunk * 2 + key_core) * chunk + k_row % chunk
            allowed = k_pos <= q_pos
            scores = jnp.where(allowed, scores, MASKED)
        old_max = row_max[...]
        new_max = jnp.maximum(old_max, jnp.max(scores, axis=1, keepdims=True))
        factor = jnp.exp2(old_max - new_max)
        weights = jnp.exp2(scores - new_max[:, :1])
        if diagonal:
            weights = jnp.where(allowed, weights, 0.0)
        row_max[...] = new_max
        row_sum[...] = row_sum[...] * factor + jnp.sum(weights, axis=1, keepdims=True)
        update = jnp.dot(weights.astype(jnp.bfloat16), lat, preferred_element_type=jnp.float32)
        acc[...] = acc[...] * factor[:, :1] + update

    def compute(k, key_core):
        first = slot_of((plane - k) * 2, 0, key_core)
        if k == 0:
            pl.when(side == 0)(lambda: attend_keys(first, 2, key_core, True))
            pl.when(side == 1)(lambda: attend_keys(first, 4, key_core, True))
        else:
            pl.when(plane >= k)(lambda: attend_keys(first, 4, key_core, False))

    def from_below(k):
        def action():
            arrived(slot_of(seq - 2 * k, pair, core), k, BELOW)
            send_corner(k)
            send_sides(k)

        when_plane(k, action)

    def from_plane(k):
        def own_side():
            index = slot_of(seq - 2 * k, other_pair, core)
            arrived(index, k, PAIR)
            send(index, k, core_peer, CORE)

        def other_side():
            for p, kind in ((pair, ACROSS), (other_pair, CORNER)):
                index = slot_of(across - 2 * k, p, core)
                arrived(index, k, kind)
                send(index, k, core_peer, CORE)

        when_plane(k, own_side)
        when_across(k, other_side)

    def from_core(k):
        first = slot_of((plane - k) * 2, 0, other_core)
        if k == 0:
            pl.when(side == 0)(lambda: arrived(first, k, CORE, 2))
            pl.when(side == 1)(lambda: arrived(first, k, CORE, 4))
        else:
            pl.when(plane >= k)(lambda: arrived(first, k, CORE, 4))

    for k in range(planes):
        if k > 0:
            from_below(k)
        if k == 1 or planes == 1:
            from_plane(0)
        if k == 2 or planes <= 2 and k == planes - 1:
            compute(0, core)
            if planes > 1:
                from_plane(1)
    for k in range(1, planes):
        from_core(k - 1)
        compute(k - 1, other_core)
        if k + 1 < planes:
            from_plane(k + 1)
        compute(k, core)
    from_core(planes - 1)
    compute(planes - 1, other_core)

    for i in range(heads):
        value_up = w_ref[:, i * (NOPE + VDIM) + NOPE:(i + 1) * (NOPE + VDIM)]
        part = slice(i * group, (i + 1) * group)
        high, low = halves(acc[part])
        result = jnp.dot(high, value_up, preferred_element_type=jnp.float32)
        result = result + jnp.dot(low, value_up, preferred_element_type=jnp.float32)
        out_ref[:, i * VDIM:(i + 1) * VDIM] = (result / row_sum[part, :VDIM]).astype(out_ref.dtype)

    for gap in range(1, planes):
        pl.when(plane + gap < planes)(lambda gap=gap: climb(gap).wait_send())
    for k in range(planes):
        copies = 7 if k else 5
        sent = copy(0, core_peer, send_sem.at[k], recv_sem.at[k, CORE], copies)
        when_plane(k, sent.wait_send)


def relay_body(queries, latent, w_kv_up):
    seq_groups = lax.axis_size("seq")
    group = queries.shape[0]
    total = group * seq_groups
    heads = w_kv_up.shape[1] // (NOPE + VDIM)
    rows = heads * group
    planes = seq_groups // 2
    return pl.pallas_call(
        functools.partial(relay_kernel, planes),
        out_shape=pltpu.VMEM((group, heads * VDIM), jnp.bfloat16),
        in_specs=[pl.BlockSpec(memory_space=pltpu.HBM)] * 3,
        out_specs=pl.BlockSpec(memory_space=pltpu.VMEM),
        scratch_shapes=[
            pltpu.VMEM((total, latent.shape[1]), jnp.bfloat16),
            pltpu.VMEM(queries.shape, jnp.bfloat16),
            pltpu.VMEM(w_kv_up.shape, jnp.bfloat16),
            pltpu.VMEM((2 * rows, D_LATENT), jnp.bfloat16),
            pltpu.VMEM((rows, ROPE), jnp.bfloat16),
            pltpu.VMEM((rows, D_LATENT), jnp.float32),
            pltpu.VMEM((rows, 128), jnp.float32),
            pltpu.VMEM((rows, 128), jnp.float32),
            pltpu.SemaphoreType.DMA((3,)),
            pltpu.SemaphoreType.DMA((planes,)),
            pltpu.SemaphoreType.DMA((planes,)),
            pltpu.SemaphoreType.DMA((planes, 5)),
            pltpu.SemaphoreType.REGULAR((planes,)),
        ],
        compiler_params=pltpu.CompilerParams(collective_id=0, has_side_effects=True),
    )(queries, latent, w_kv_up)


def solution(mesh):
    in_specs = (P("seq", "head"), P(("seq", "head"), None), P(None, "head"))
    out_specs = P("seq", "head")
    small = mesh.shape["seq"] <= 16 and mesh.shape["seq"] % 2 == 0 and mesh.shape["head"] == 4
    chosen = relay_body if small else body
    return jax.shard_map(chosen, mesh=mesh, in_specs=in_specs, out_specs=out_specs, check_vma=False)
```

```python
import functools
import math

import jax
import jax.numpy as jnp
from jax import lax
from jax.experimental import pallas as pl
from jax.experimental.pallas import tpu as pltpu
from jax.sharding import PartitionSpec as P

D_LATENT = 256
ROPE = 64
NOPE = 128
VDIM = 128


MASKED = -1e30


def from_behind(shard, axis, by):
    length = lax.axis_size(axis)
    pairs = [(i, i + by) for i in range(length) if 0 <= i + by < length]
    return lax.ppermute(shard, axis, pairs)


def attend(state, key_block, key_start, setup):
    query_side, query_rope, query_pos, w_kv_up, absorb = setup
    numerator, running_max, totals = state
    local_heads = query_rope.shape[1]
    key_count = key_block.shape[0]
    highest = lax.Precision.HIGHEST
    key_latent = key_block[:, :D_LATENT]
    key_rope = key_block[:, D_LATENT:]
    key_value = jnp.dot(key_latent, w_kv_up, preferred_element_type=jnp.float32)
    key_value = key_value.reshape(key_count, local_heads, NOPE + VDIM)
    scores = jnp.einsum("qhd,khd->hqk", query_side, key_value[:, :, :NOPE], precision=highest)
    scores = scores + jnp.einsum(
        "qhd,kd->hqk", query_rope, key_rope, preferred_element_type=jnp.float32
    )
    scores = scores * (NOPE + ROPE) ** (-0.5)
    key_pos = key_start + lax.iota(jnp.int32, key_count)
    allowed = (key_pos[None, :] <= query_pos[:, None]) & (key_pos[None, :] >= 0)
    scores = jnp.where(allowed[None], scores, MASKED)
    new_max = jnp.maximum(running_max, jnp.max(scores, axis=2))
    factor = jnp.exp(running_max - new_max)
    weights = jnp.where(allowed[None], jnp.exp(scores - new_max[:, :, None]), 0.0)
    totals = totals * factor + jnp.sum(weights, axis=2)
    rounded = weights.astype(jnp.bfloat16)
    update = jnp.einsum(
        "hqk,khd->hqd", rounded.astype(jnp.float32), key_value[:, :, NOPE:], precision=highest
    )
    numerator = numerator * factor[:, :, None] + update
    return (numerator, new_max, totals)


def attend_blocks(state, keys, key_start, setup):
    key_total = keys.shape[0]
    block_rows = key_total if key_total <= 1024 else math.gcd(key_total, 1024)
    block_count = key_total // block_rows

    def one_block(block_index, inner):
        offset = block_index * block_rows
        piece = lax.dynamic_slice_in_dim(keys, offset, block_rows, 0)
        return attend(inner, piece, key_start + offset, setup)

    if block_count == 1:
        return one_block(0, state)
    return lax.fori_loop(0, block_count, one_block, state)


def prepare(query_rows, query_pos, w_kv_up):
    row_count = query_rows.shape[0]
    local_heads = w_kv_up.shape[1] // (NOPE + VDIM)
    query_all = query_rows.reshape(row_count, local_heads, NOPE + ROPE)
    query_side = query_all[:, :, :NOPE].astype(jnp.float32)
    width = VDIM
    setup = (query_side, query_all[:, :, NOPE:], query_pos, w_kv_up, False)
    start_state = (
        jnp.zeros((local_heads, row_count, width), jnp.float32),
        jnp.full((local_heads, row_count), MASKED, jnp.float32),
        jnp.zeros((local_heads, row_count), jnp.float32),
    )
    return (setup, start_state)


def finish(state, w_kv_up):
    numerator, running_max, totals = state
    local_heads = w_kv_up.shape[1] // (NOPE + VDIM)
    row_count = totals.shape[1]
    result = numerator / totals[:, :, None]
    return (
        jnp.transpose(result, (1, 0, 2)).reshape(row_count, local_heads * VDIM).astype(jnp.bfloat16)
    )


def body(queries, latent, w_kv_up):
    group_rows = queries.shape[0]
    seq_groups = lax.axis_size("seq")
    group_index = lax.axis_index("seq")
    query_pos = group_index * group_rows + lax.iota(jnp.int32, group_rows)
    setup, state = prepare(queries, query_pos, w_kv_up)
    gathered = lax.all_gather(latent, "head", axis=0, tiled=True)
    state = attend(state, gathered, group_index * group_rows, setup)
    history = gathered
    span_groups = 1
    while span_groups < seq_groups:
        arrived = from_behind(history, "seq", span_groups)
        state = attend_blocks(
            state, arrived, (group_index - 2 * span_groups + 1) * group_rows, setup
        )
        if 2 * span_groups < seq_groups:
            history = jnp.concatenate([arrived, history], axis=0)
        span_groups = span_groups * 2
    return finish(state, w_kv_up)


LOG2E = 1.4426950408889634
MESH = pl.DeviceIdType.MESH
def dot_rows(a, b):
    return lax.dot_general(a, b, (((1,), (1,)), ((), ())), preferred_element_type=jnp.float32)


def halves(x):
    high = x.astype(jnp.bfloat16)
    low = (x - high.astype(jnp.float32)).astype(jnp.bfloat16)
    return high, low


def across_lanes(column, width):
    repeats = -(-width // column.shape[1])
    return jnp.concatenate([column] * repeats, axis=1)[:, :width]


def relay_kernel(
    planes, q_hbm, lat_hbm, w_hbm, out_ref,
    keys, q_ref, w_ref, absorbed, rope, acc, row_max, row_sum,
    load_sem, climb_sem, send_sem, recv_sem, ready_sem,
):
    seq, hd = lax.axis_index("seq"), lax.axis_index("head")
    plane, side = seq // 2, seq % 2
    pair, core = hd // 2, hd % 2
    chunk = lat_hbm.shape[0]
    group = q_ref.shape[0]
    heads = w_ref.shape[1] // (NOPE + VDIM)
    across = seq + 1 - 2 * side
    other_pair = 1 - pair
    other_core = 1 - core

    def slot_of(s, p, c):
        return (c * planes * 2 + s) * 2 + p

    def region(index, count):
        return keys.at[pl.ds(pl.multiple_of(index * chunk, chunk), count * chunk)]

    def copy(index, target, sent, landed, count=1):
        return pltpu.make_async_remote_copy(
            src_ref=region(index, count),
            dst_ref=region(index, count),
            send_sem=sent,
            recv_sem=landed,
            device_id=target,
            device_id_type=MESH,
        )

    own = slot_of(seq, pair, core)
    own_rows = pl.ds(pl.multiple_of(own * chunk, chunk), chunk)
    load_own = pltpu.make_async_copy(lat_hbm, keys.at[own_rows], load_sem.at[0])
    load_q = pltpu.make_async_copy(q_hbm, q_ref, load_sem.at[1])
    load_w = pltpu.make_async_copy(w_hbm, w_ref, load_sem.at[2])
    load_own.start()

    across_peer = (across, hd)
    pair_peer = (seq, other_pair * 2 + core)
    corner_peer = (across, other_pair * 2 + core)
    core_peer = (seq, pair * 2 + other_core)
    below, above = (seq - 2, hd), (seq + 2, hd)
    has_below, has_above = plane > 0, plane < planes - 1

    barrier = pltpu.get_barrier_semaphore()

    @pl.when(has_below)
    def _():
        pl.semaphore_signal(barrier, inc=1, device_id=below, device_id_type=MESH)

    for target in (pair_peer, across_peer, core_peer):
        pl.semaphore_signal(barrier, inc=1, device_id=target, device_id_type=MESH)

    @pl.when(has_above)
    def _():
        pl.semaphore_signal(barrier, inc=1, device_id=above, device_id_type=MESH)

    load_q.start()
    load_w.start()
    pl.semaphore_wait(barrier, 3 + jnp.where(has_below, 1, 0) + jnp.where(has_above, 1, 0))

    def pass_down(gap):
        pl.semaphore_signal(ready_sem.at[gap], inc=1, device_id=below, device_id_type=MESH)

    if planes > 2:
        pl.when(has_below & has_above)(lambda: pass_down(2))
    pl.semaphore_signal(ready_sem.at[0], inc=1, device_id=pair_peer, device_id_type=MESH)

    def guarded(condition, action):
        if condition is True:
            action()
        else:
            pl.when(condition)(action)

    BELOW, PAIR, ACROSS, CORNER, CORE = range(5)

    def climb(gap):
        return copy(own, (seq + 2 * gap, hd), climb_sem.at[gap], recv_sem.at[gap, BELOW])

    def send(index, k, target, kind):
        copy(index, target, send_sem.at[k], recv_sem.at[k, kind]).start()

    def send_sides(k):
        index = slot_of(seq - 2 * k, pair, core)
        guarded(True if k else side == 0, lambda: send(index, k, across_peer, ACROSS))
        send(index, k, pair_peer, PAIR)
        send(index, k, core_peer, CORE)

    def send_corner(k):
        index = slot_of(seq - 2 * k, pair, core)
        guarded(True if k else side == 0, lambda: send(index, k, corner_peer, CORNER))

    def arrived(index, k, kind, count=1):
        copy(index, core_peer, send_sem.at[k], recv_sem.at[k, kind], count).wait_recv()

    def when_plane(k, action):
        guarded(True if k == 0 else plane >= k, action)

    def when_across(k, action):
        guarded(side == 1 if k == 0 else plane >= k, action)

    load_own.wait()
    if planes > 1:
        pl.when(has_above)(lambda: climb(1).start())
    send_sides(0)
    pl.semaphore_wait(ready_sem.at[0], 1)
    send_corner(0)
    for gap in range(2, planes):
        @pl.when(plane + gap < planes)
        def _(gap=gap):
            pl.semaphore_wait(ready_sem.at[gap], 1)
            if gap + 1 < planes:
                pl.when(has_below)(lambda: pass_down(gap + 1))
            climb(gap).start()

    load_q.wait()
    load_w.wait()
    for i in range(heads):
        left = i * (NOPE + ROPE)
        key_up = w_ref[:, i * (NOPE + VDIM):i * (NOPE + VDIM) + NOPE]
        mixed = dot_rows(q_ref[:, left:left + NOPE], key_up)
        high, low = halves(mixed)
        absorbed[i * group:(i + 1) * group] = high
        absorbed[(heads + i) * group:(heads + i + 1) * group] = low
        rope[i * group:(i + 1) * group] = q_ref[:, left + NOPE:left + NOPE + ROPE]
    row_max[...] = jnp.full_like(row_max, MASKED)
    row_sum[...] = jnp.zeros_like(row_sum)
    acc[...] = jnp.zeros_like(acc)

    scale = LOG2E * (NOPE + ROPE) ** (-0.5)
    rows = heads * group

    def attend_keys(first_slot, slots, key_core, diagonal):
        count = slots * chunk
        block = pl.ds(pl.multiple_of(first_slot * chunk, chunk), count)
        lat = keys[block, :D_LATENT]
        both = dot_rows(absorbed[...], lat)
        scores = both[:rows] + both[rows:] + dot_rows(rope[...], keys[block, D_LATENT:])
        scores = scores * scale
        if diagonal:
            q_pos = lax.broadcasted_iota(jnp.int32, (rows, count), 0) % group
            q_pos = q_pos + (slots // 2 - 1) * group
            k_row = lax.broadcasted_iota(jnp.int32, (rows, count), 1)
            k_pos = (k_row // chunk * 2 + key_core) * chunk + k_row % chunk
            allowed = k_pos <= q_pos
            scores = jnp.where(allowed, scores, MASKED)
        old_max = row_max[...]
        new_max = jnp.maximum(old_max, jnp.max(scores, axis=1, keepdims=True))
        factor = jnp.exp2(old_max - new_max)
        weights = jnp.exp2(scores - across_lanes(new_max, count))
        if diagonal:
            weights = jnp.where(allowed, weights, 0.0)
        row_max[...] = new_max
        row_sum[...] = row_sum[...] * factor + jnp.sum(weights, axis=1, keepdims=True)
        update = jnp.dot(weights.astype(jnp.bfloat16), lat, preferred_element_type=jnp.float32)
        acc[...] = acc[...] * across_lanes(factor, D_LATENT) + update

    def compute(k, key_core):
        first = slot_of((plane - k) * 2, 0, key_core)
        if k == 0:
            pl.when(side == 0)(lambda: attend_keys(first, 2, key_core, True))
            pl.when(side == 1)(lambda: attend_keys(first, 4, key_core, True))
        else:
            pl.when(plane >= k)(lambda: attend_keys(first, 4, key_core, False))

    def from_below(k):
        def action():
            arrived(slot_of(seq - 2 * k, pair, core), k, BELOW)
            send_corner(k)
            send_sides(k)

        when_plane(k, action)

    def from_plane(k):
        def own_side():
            index = slot_of(seq - 2 * k, other_pair, core)
            arrived(index, k, PAIR)
            send(index, k, core_peer, CORE)

        def other_side():
            for p, kind in ((pair, ACROSS), (other_pair, CORNER)):
                index = slot_of(across - 2 * k, p, core)
                arrived(index, k, kind)
                send(index, k, core_peer, CORE)

        when_plane(k, own_side)
        when_across(k, other_side)

    def from_core(k):
        first = slot_of((plane - k) * 2, 0, other_core)
        if k == 0:
            pl.when(side == 0)(lambda: arrived(first, k, CORE, 2))
            pl.when(side == 1)(lambda: arrived(first, k, CORE, 4))
        else:
            pl.when(plane >= k)(lambda: arrived(first, k, CORE, 4))

    for k in range(planes):
        if k > 0:
            from_below(k)
        if 1 <= k <= 2:
            from_plane(k - 1)
    for k in range(min(planes - 1, 2), min(planes, 2)):
        from_plane(k)
    compute(0, core)
    for k in range(planes):
        from_core(k)
        compute(k, other_core)
        ahead = k + 2
        if ahead < planes:
            from_plane(ahead)
        if k + 1 < planes:
            compute(k + 1, core)

    for i in range(heads):
        value_up = w_ref[:, i * (NOPE + VDIM) + NOPE:(i + 1) * (NOPE + VDIM)]
        part = slice(i * group, (i + 1) * group)
        high, low = halves(acc[part])
        result = jnp.dot(high, value_up, preferred_element_type=jnp.float32)
        result = result + jnp.dot(low, value_up, preferred_element_type=jnp.float32)
        out_ref[:, i * VDIM:(i + 1) * VDIM] = (result / row_sum[part, :VDIM]).astype(out_ref.dtype)

    for gap in range(1, planes):
        pl.when(plane + gap < planes)(lambda gap=gap: climb(gap).wait_send())
    for k in range(planes):
        copies = 7 if k else 5
        sent = copy(0, core_peer, send_sem.at[k], recv_sem.at[k, CORE], copies)
        when_plane(k, sent.wait_send)


def relay_body(queries, latent, w_kv_up):
    seq_groups = lax.axis_size("seq")
    group = queries.shape[0]
    total = group * seq_groups
    heads = w_kv_up.shape[1] // (NOPE + VDIM)
    rows = heads * group
    planes = seq_groups // 2
    return pl.pallas_call(
        functools.partial(relay_kernel, planes),
        out_shape=pltpu.VMEM((group, heads * VDIM), jnp.bfloat16),
        in_specs=[pl.BlockSpec(memory_space=pltpu.HBM)] * 3,
        out_specs=pl.BlockSpec(memory_space=pltpu.VMEM),
        scratch_shapes=[
            pltpu.VMEM((total, latent.shape[1]), jnp.bfloat16),
            pltpu.VMEM(queries.shape, jnp.bfloat16),
            pltpu.VMEM(w_kv_up.shape, jnp.bfloat16),
            pltpu.VMEM((2 * rows, D_LATENT), jnp.bfloat16),
            pltpu.VMEM((rows, ROPE), jnp.bfloat16),
            pltpu.VMEM((rows, D_LATENT), jnp.float32),
            pltpu.VMEM((rows, 128), jnp.float32),
            pltpu.VMEM((rows, 128), jnp.float32),
            pltpu.SemaphoreType.DMA((3,)),
            pltpu.SemaphoreType.DMA((planes,)),
            pltpu.SemaphoreType.DMA((planes,)),
            pltpu.SemaphoreType.DMA((planes, 5)),
            pltpu.SemaphoreType.REGULAR((planes,)),
        ],
        compiler_params=pltpu.CompilerParams(collective_id=0, has_side_effects=True),
    )(queries, latent, w_kv_up)


def solution(mesh):
    in_specs = (P("seq", "head"), P(("seq", "head"), None), P(None, "head"))
    out_specs = P("seq", "head")
    small = mesh.shape["seq"] <= 16 and mesh.shape["seq"] % 2 == 0 and mesh.shape["head"] == 4
    chosen = relay_body if small else body
    return jax.shard_map(chosen, mesh=mesh, in_specs=in_specs, out_specs=out_specs, check_vma=False)
```

```python
import functools
import math

import jax
import jax.numpy as jnp
from jax import lax
from jax.experimental import pallas as pl
from jax.experimental.pallas import tpu as pltpu
from jax.sharding import PartitionSpec as P

D_LATENT = 256
ROPE = 64
NOPE = 128
VDIM = 128


MASKED = -1e30


def from_behind(shard, axis, by):
    length = lax.axis_size(axis)
    pairs = [(i, i + by) for i in range(length) if 0 <= i + by < length]
    return lax.ppermute(shard, axis, pairs)


def attend(state, key_block, key_start, setup):
    query_side, query_rope, query_pos, w_kv_up, absorb = setup
    numerator, running_max, totals = state
    local_heads = query_rope.shape[1]
    key_count = key_block.shape[0]
    highest = lax.Precision.HIGHEST
    key_latent = key_block[:, :D_LATENT]
    key_rope = key_block[:, D_LATENT:]
    key_value = jnp.dot(key_latent, w_kv_up, preferred_element_type=jnp.float32)
    key_value = key_value.reshape(key_count, local_heads, NOPE + VDIM)
    scores = jnp.einsum("qhd,khd->hqk", query_side, key_value[:, :, :NOPE], precision=highest)
    scores = scores + jnp.einsum(
        "qhd,kd->hqk", query_rope, key_rope, preferred_element_type=jnp.float32
    )
    scores = scores * (NOPE + ROPE) ** (-0.5)
    key_pos = key_start + lax.iota(jnp.int32, key_count)
    allowed = (key_pos[None, :] <= query_pos[:, None]) & (key_pos[None, :] >= 0)
    scores = jnp.where(allowed[None], scores, MASKED)
    new_max = jnp.maximum(running_max, jnp.max(scores, axis=2))
    factor = jnp.exp(running_max - new_max)
    weights = jnp.where(allowed[None], jnp.exp(scores - new_max[:, :, None]), 0.0)
    totals = totals * factor + jnp.sum(weights, axis=2)
    rounded = weights.astype(jnp.bfloat16)
    update = jnp.einsum(
        "hqk,khd->hqd", rounded.astype(jnp.float32), key_value[:, :, NOPE:], precision=highest
    )
    numerator = numerator * factor[:, :, None] + update
    return (numerator, new_max, totals)


def attend_blocks(state, keys, key_start, setup):
    key_total = keys.shape[0]
    block_rows = key_total if key_total <= 1024 else math.gcd(key_total, 1024)
    block_count = key_total // block_rows

    def one_block(block_index, inner):
        offset = block_index * block_rows
        piece = lax.dynamic_slice_in_dim(keys, offset, block_rows, 0)
        return attend(inner, piece, key_start + offset, setup)

    if block_count == 1:
        return one_block(0, state)
    return lax.fori_loop(0, block_count, one_block, state)


def prepare(query_rows, query_pos, w_kv_up):
    row_count = query_rows.shape[0]
    local_heads = w_kv_up.shape[1] // (NOPE + VDIM)
    query_all = query_rows.reshape(row_count, local_heads, NOPE + ROPE)
    query_side = query_all[:, :, :NOPE].astype(jnp.float32)
    width = VDIM
    setup = (query_side, query_all[:, :, NOPE:], query_pos, w_kv_up, False)
    start_state = (
        jnp.zeros((local_heads, row_count, width), jnp.float32),
        jnp.full((local_heads, row_count), MASKED, jnp.float32),
        jnp.zeros((local_heads, row_count), jnp.float32),
    )
    return (setup, start_state)


def finish(state, w_kv_up):
    numerator, running_max, totals = state
    local_heads = w_kv_up.shape[1] // (NOPE + VDIM)
    row_count = totals.shape[1]
    result = numerator / totals[:, :, None]
    return (
        jnp.transpose(result, (1, 0, 2)).reshape(row_count, local_heads * VDIM).astype(jnp.bfloat16)
    )


def body(queries, latent, w_kv_up):
    group_rows = queries.shape[0]
    seq_groups = lax.axis_size("seq")
    group_index = lax.axis_index("seq")
    query_pos = group_index * group_rows + lax.iota(jnp.int32, group_rows)
    setup, state = prepare(queries, query_pos, w_kv_up)
    gathered = lax.all_gather(latent, "head", axis=0, tiled=True)
    state = attend(state, gathered, group_index * group_rows, setup)
    history = gathered
    span_groups = 1
    while span_groups < seq_groups:
        arrived = from_behind(history, "seq", span_groups)
        state = attend_blocks(
            state, arrived, (group_index - 2 * span_groups + 1) * group_rows, setup
        )
        if 2 * span_groups < seq_groups:
            history = jnp.concatenate([arrived, history], axis=0)
        span_groups = span_groups * 2
    return finish(state, w_kv_up)


LOG2E = 1.4426950408889634
MESH = pl.DeviceIdType.MESH
def dot_rows(a, b):
    return lax.dot_general(a, b, (((1,), (1,)), ((), ())), preferred_element_type=jnp.float32)


def halves(x):
    high = x.astype(jnp.bfloat16)
    low = (x - high.astype(jnp.float32)).astype(jnp.bfloat16)
    return high, low


def across_lanes(column, width):
    repeats = -(-width // column.shape[1])
    return jnp.concatenate([column] * repeats, axis=1)[:, :width]


def relay_kernel(
    planes, q_hbm, lat_hbm, w_hbm, out_ref,
    keys, q_ref, w_ref, absorbed, rope, acc, row_max, row_sum,
    load_sem, climb_sem, send_sem, recv_sem, ready_sem,
):
    seq, hd = lax.axis_index("seq"), lax.axis_index("head")
    plane, side = seq // 2, seq % 2
    pair, core = hd // 2, hd % 2
    chunk = lat_hbm.shape[0]
    group = q_ref.shape[0]
    heads = w_ref.shape[1] // (NOPE + VDIM)
    across = seq + 1 - 2 * side
    other_pair = 1 - pair
    other_core = 1 - core

    def slot_of(s, p, c):
        return (c * planes * 2 + s) * 2 + p

    def region(index, count):
        return keys.at[pl.ds(pl.multiple_of(index * chunk, chunk), count * chunk)]

    def copy(index, target, sent, landed, count=1):
        return pltpu.make_async_remote_copy(
            src_ref=region(index, count),
            dst_ref=region(index, count),
            send_sem=sent,
            recv_sem=landed,
            device_id=target,
            device_id_type=MESH,
        )

    own = slot_of(seq, pair, core)
    own_rows = pl.ds(pl.multiple_of(own * chunk, chunk), chunk)
    load_own = pltpu.make_async_copy(lat_hbm, keys.at[own_rows], load_sem.at[0])
    load_q = pltpu.make_async_copy(q_hbm, q_ref, load_sem.at[1])
    load_w = pltpu.make_async_copy(w_hbm, w_ref, load_sem.at[2])
    load_own.start()

    across_peer = (across, hd)
    pair_peer = (seq, other_pair * 2 + core)
    corner_peer = (across, other_pair * 2 + core)
    core_peer = (seq, pair * 2 + other_core)
    below, above = (seq - 2, hd), (seq + 2, hd)
    has_below, has_above = plane > 0, plane < planes - 1

    barrier = pltpu.get_barrier_semaphore()

    @pl.when(has_below)
    def _():
        pl.semaphore_signal(barrier, inc=1, device_id=below, device_id_type=MESH)

    for target in (pair_peer, across_peer, core_peer):
        pl.semaphore_signal(barrier, inc=1, device_id=target, device_id_type=MESH)

    @pl.when(has_above)
    def _():
        pl.semaphore_signal(barrier, inc=1, device_id=above, device_id_type=MESH)

    load_q.start()
    load_w.start()
    pl.semaphore_wait(barrier, 3 + jnp.where(has_below, 1, 0) + jnp.where(has_above, 1, 0))

    def pass_down(gap):
        pl.semaphore_signal(ready_sem.at[gap], inc=1, device_id=below, device_id_type=MESH)

    if planes > 2:
        pl.when(has_below & has_above)(lambda: pass_down(2))
    pl.semaphore_signal(ready_sem.at[0], inc=1, device_id=pair_peer, device_id_type=MESH)

    def guarded(condition, action):
        if condition is True:
            action()
        else:
            pl.when(condition)(action)

    BELOW, PAIR, ACROSS, CORNER, CORE = range(5)

    def climb(gap):
        return copy(own, (seq + 2 * gap, hd), climb_sem.at[gap], recv_sem.at[gap, BELOW])

    def send(index, k, target, kind):
        copy(index, target, send_sem.at[k], recv_sem.at[k, kind]).start()

    def send_sides(k):
        index = slot_of(seq - 2 * k, pair, core)
        guarded(True if k else side == 0, lambda: send(index, k, across_peer, ACROSS))
        send(index, k, pair_peer, PAIR)
        send(index, k, core_peer, CORE)

    def send_corner(k):
        index = slot_of(seq - 2 * k, pair, core)
        guarded(True if k else side == 0, lambda: send(index, k, corner_peer, CORNER))

    def arrived(index, k, kind, count=1):
        copy(index, core_peer, send_sem.at[k], recv_sem.at[k, kind], count).wait_recv()

    def when_plane(k, action):
        guarded(True if k == 0 else plane >= k, action)

    def when_across(k, action):
        guarded(side == 1 if k == 0 else plane >= k, action)

    load_own.wait()
    if planes > 1:
        pl.when(has_above)(lambda: climb(1).start())
    send_sides(0)
    pl.semaphore_wait(ready_sem.at[0], 1)
    send_corner(0)
    for gap in range(2, planes):
        @pl.when(plane + gap < planes)
        def _(gap=gap):
            pl.semaphore_wait(ready_sem.at[gap], 1)
            if gap + 1 < planes:
                pl.when(has_below)(lambda: pass_down(gap + 1))
            climb(gap).start()

    load_q.wait()
    load_w.wait()
    for i in range(heads):
        left = i * (NOPE + ROPE)
        key_up = w_ref[:, i * (NOPE + VDIM):i * (NOPE + VDIM) + NOPE]
        mixed = dot_rows(q_ref[:, left:left + NOPE], key_up)
        high, low = halves(mixed)
        absorbed[i * group:(i + 1) * group] = high
        absorbed[(heads + i) * group:(heads + i + 1) * group] = low
        rope[i * group:(i + 1) * group] = q_ref[:, left + NOPE:left + NOPE + ROPE]
    row_max[...] = jnp.full_like(row_max, MASKED)
    row_sum[...] = jnp.zeros_like(row_sum)
    acc[...] = jnp.zeros_like(acc)

    scale = LOG2E * (NOPE + ROPE) ** (-0.5)
    rows = heads * group

    def attend_keys(first_slot, slots, key_core, diagonal):
        count = slots * chunk
        block = pl.ds(pl.multiple_of(first_slot * chunk, chunk), count)
        lat = keys[block, :D_LATENT]
        both = dot_rows(absorbed[...], lat)
        scores = both[:rows] + both[rows:] + dot_rows(rope[...], keys[block, D_LATENT:])
        scores = scores * scale
        if diagonal:
            q_pos = lax.broadcasted_iota(jnp.int32, (rows, count), 0) % group
            q_pos = q_pos + (slots // 2 - 1) * group
            k_row = lax.broadcasted_iota(jnp.int32, (rows, count), 1)
            k_pos = (k_row // chunk * 2 + key_core) * chunk + k_row % chunk
            allowed = k_pos <= q_pos
            scores = jnp.where(allowed, scores, MASKED)
        old_max = row_max[...]
        new_max = jnp.maximum(old_max, jnp.max(scores, axis=1, keepdims=True))
        factor = jnp.exp2(old_max - new_max)
        weights = jnp.exp2(scores - across_lanes(new_max, count))
        if diagonal:
            weights = jnp.where(allowed, weights, 0.0)
        row_max[...] = new_max
        row_sum[...] = row_sum[...] * factor + jnp.sum(weights, axis=1, keepdims=True)
        update = jnp.dot(weights.astype(jnp.bfloat16), lat, preferred_element_type=jnp.float32)
        acc[...] = acc[...] * across_lanes(factor, D_LATENT) + update

    def compute(k, key_core):
        first = slot_of((plane - k) * 2, 0, key_core)
        if k == 0:
            pl.when(side == 0)(lambda: attend_keys(first, 2, key_core, True))
            pl.when(side == 1)(lambda: attend_keys(first, 4, key_core, True))
        else:
            pl.when(plane >= k)(lambda: attend_keys(first, 4, key_core, False))

    def from_below(k):
        def action():
            arrived(slot_of(seq - 2 * k, pair, core), k, BELOW)
            send_corner(k)
            send_sides(k)

        when_plane(k, action)

    def from_plane(k):
        def own_side():
            index = slot_of(seq - 2 * k, other_pair, core)
            arrived(index, k, PAIR)
            send(index, k, core_peer, CORE)

        def other_side():
            for p, kind in ((pair, ACROSS), (other_pair, CORNER)):
                index = slot_of(across - 2 * k, p, core)
                arrived(index, k, kind)
                send(index, k, core_peer, CORE)

        when_plane(k, own_side)
        when_across(k, other_side)

    def from_core(k):
        first = slot_of((plane - k) * 2, 0, other_core)
        if k == 0:
            pl.when(side == 0)(lambda: arrived(first, k, CORE, 2))
            pl.when(side == 1)(lambda: arrived(first, k, CORE, 4))
        else:
            pl.when(plane >= k)(lambda: arrived(first, k, CORE, 4))

    def attend_first():
        compute(0, core)
        from_core(0)
        compute(0, other_core)

    for k in range(planes):
        if k > 0:
            from_below(k)
        if 1 <= k <= 2:
            if k == 2:
                attend_first()
            from_plane(k - 1)
    if planes < 3:
        for k in range(planes - 1, planes):
            from_plane(k)
        attend_first()
    for k in range(1, planes):
        compute(k, core)
        if k + 1 < planes and k + 1 >= 2:
            from_plane(k + 1)
        from_core(k)
        compute(k, other_core)

    for i in range(heads):
        value_up = w_ref[:, i * (NOPE + VDIM) + NOPE:(i + 1) * (NOPE + VDIM)]
        part = slice(i * group, (i + 1) * group)
        high, low = halves(acc[part])
        result = jnp.dot(high, value_up, preferred_element_type=jnp.float32)
        result = result + jnp.dot(low, value_up, preferred_element_type=jnp.float32)
        out_ref[:, i * VDIM:(i + 1) * VDIM] = (result / row_sum[part, :VDIM]).astype(out_ref.dtype)

    for gap in range(1, planes):
        pl.when(plane + gap < planes)(lambda gap=gap: climb(gap).wait_send())
    for k in range(planes):
        copies = 7 if k else 5
        sent = copy(0, core_peer, send_sem.at[k], recv_sem.at[k, CORE], copies)
        when_plane(k, sent.wait_send)


def relay_body(queries, latent, w_kv_up):
    seq_groups = lax.axis_size("seq")
    group = queries.shape[0]
    total = group * seq_groups
    heads = w_kv_up.shape[1] // (NOPE + VDIM)
    rows = heads * group
    planes = seq_groups // 2
    return pl.pallas_call(
        functools.partial(relay_kernel, planes),
        out_shape=pltpu.VMEM((group, heads * VDIM), jnp.bfloat16),
        in_specs=[pl.BlockSpec(memory_space=pltpu.HBM)] * 3,
        out_specs=pl.BlockSpec(memory_space=pltpu.VMEM),
        scratch_shapes=[
            pltpu.VMEM((total, latent.shape[1]), jnp.bfloat16),
            pltpu.VMEM(queries.shape, jnp.bfloat16),
            pltpu.VMEM(w_kv_up.shape, jnp.bfloat16),
            pltpu.VMEM((2 * rows, D_LATENT), jnp.bfloat16),
            pltpu.VMEM((rows, ROPE), jnp.bfloat16),
            pltpu.VMEM((rows, D_LATENT), jnp.float32),
            pltpu.VMEM((rows, 128), jnp.float32),
            pltpu.VMEM((rows, 128), jnp.float32),
            pltpu.SemaphoreType.DMA((3,)),
            pltpu.SemaphoreType.DMA((planes,)),
            pltpu.SemaphoreType.DMA((planes,)),
            pltpu.SemaphoreType.DMA((planes, 5)),
            pltpu.SemaphoreType.REGULAR((planes,)),
        ],
        compiler_params=pltpu.CompilerParams(collective_id=0, has_side_effects=True),
    )(queries, latent, w_kv_up)


def solution(mesh):
    in_specs = (P("seq", "head"), P(("seq", "head"), None), P(None, "head"))
    out_specs = P("seq", "head")
    small = mesh.shape["seq"] <= 16 and mesh.shape["seq"] % 2 == 0 and mesh.shape["head"] == 4
    chosen = relay_body if small else body
    return jax.shard_map(chosen, mesh=mesh, in_specs=in_specs, out_specs=out_specs, check_vma=False)
```
